256 devices in a mesh: layer: 8 (over y, z_lo), lat: 4 (over x), tok: 8 (over z_hi, core).
Axes of the slice: x: 4, y: 4, z: 8 (z_hi: 4, z_lo: 2; z = z_hi * 2 + z_lo), core: 2. Of those that a mesh axis runs over, the one named last changes fastest.
Arguments:
- mlp_inputs: bfloat16 [8, 768, 4096], P('layer', ('lat', 'tok')), may hold values from -6 to 6
- mlp_outputs: bfloat16 [8, 768, 4096], P('layer', ('lat', 'tok')), may hold values from -6 to 6
- encoder: bfloat16 [8, 4096, 16384], P('layer', None, ('lat', 'tok')), may hold values from -0.09375 to 0.09375
- encoder_bias: float32 [8, 16384], P('layer', ('lat', 'tok')), may hold values from -3 to 3
- active_words: int32 [8, 768, 1024], P('layer', None, ('lat', 'tok')), may hold values from 0 to 65535
- decoder: bfloat16 [8, 16384, 4096], P('layer', ('lat', 'tok')), may hold values from -0.0234375 to 0.0234375
Outputs:
- reconstruction_error: bfloat16 [8, 768, 4096], P('layer', ('lat', 'tok'))
- decoder_grad: bfloat16 [8, 16384, 4096], P('layer', ('lat', 'tok'))
The draws below stay inside these ranges and needn't reach their ends.
Inputs may be any that keep to these rules, and one draw needn't show every extreme that they name: `active_words`: each word holds 16 independent gate decisions of one token in its low 16 bits.
All inputs are finite; a program needn't handle non-finite values.
Results may differ from the reference program's by a relative error of at most 0.0037.
Values may be sent and summed in bfloat16 or wider, within the bound.
No kernel may reach another device: no remote copies, remote signals or barrier semaphores. Data moves between devices by JAX's collectives and lax.ppermute only.
A program may use at most 128 MiB of HBM per device.

```python
import jax
import jax.numpy as jnp

D = 4096
F = 16384
L = 8
TOKENS = 768


def plant(drawn, own_key, least, largest):
    index_at = [jax.random.randint(jax.random.fold_in(own_key, axis), (), 0, length) for axis, length in enumerate(drawn.shape)]
    main_axis = drawn.shape.index(max(drawn.shape))
    next_to = index_at[:main_axis] + [(index_at[main_axis] + 1) % drawn.shape[main_axis]] + index_at[main_axis + 1:]
    return drawn.at[tuple(index_at)].set(least).at[tuple(next_to)].set(largest)


def block_levels(key, extent, cuts, low, top_value):
    def one(position, shards_of):
        heights = jax.random.uniform(jax.random.fold_in(jax.random.fold_in(key, 6), position), (shards_of,), jnp.float32, low / len(cuts), top_value / len(cuts))
        return jnp.repeat(jnp.exp(heights), extent[position] // shards_of).reshape((-1,) + (1,) * (len(extent) - position - 1))

    factor_of = one(*cuts[0])
    for cut in cuts[1:]:
        factor_of = factor_of * one(*cut)
    return factor_of


def normal_values(rng, shape, spread, limit, pieces=(), held_as=jnp.bfloat16):
    result = spread * jax.random.normal(rng, shape, jnp.float32)
    if pieces:
        result = result * block_levels(rng, shape, pieces, -0.22, 0.18)
    return jnp.clip(result, -limit, limit).astype(held_as)


def setup_inputs(seed: int = 0) -> dict:
    splits = jax.random.split(jax.random.key(seed), 7)
    return {
        "mlp_inputs": normal_values(splits[0], (L, TOKENS, D), 1.0, 6.0, ((0, 8), (1, 32))),
        "mlp_outputs": normal_values(splits[1], (L, TOKENS, D), 1.0, 6.0, ((0, 8), (1, 32))),
        "encoder": normal_values(splits[2], (L, D, F), D ** -0.5, 0.09375, ((0, 8), (2, 32))),
        "encoder_bias": normal_values(splits[3], (L, F), 0.5, 3.0, ((0, 8), (1, 32)), jnp.float32),
        "active_words": plant(jax.random.randint(splits[4], (L, TOKENS, F // 16), 0, 65536), jax.random.fold_in(splits[4], 1), 0, 65535).astype(jnp.int32),
        "decoder": normal_values(splits[5], (L, F, D), (4 * F) ** -0.5, 0.0234375, ((0, 8), (1, 32))),
    }


def unpack_words(words):
    shifts = jnp.arange(16, dtype=jnp.int32)
    bits = jnp.right_shift(words[..., None], shifts) & 1
    return bits.reshape(words.shape[:-1] + (words.shape[-1] * 16,)).astype(jnp.float32)


def reference(mlp_inputs, mlp_outputs, encoder, encoder_bias, active_words, decoder):
    latents = []
    writes = []
    for layer in range(L):
        before_gate = jnp.dot(mlp_inputs[layer], encoder[layer], preferred_element_type=jnp.float32)
        before_gate = before_gate + encoder_bias[layer].astype(jnp.float32)[None, :]
        latent = (unpack_words(active_words[layer]) * before_gate).astype(jnp.bfloat16)
        latents.append(latent)
        writes.append(jnp.dot(latent, decoder[layer], preferred_element_type=jnp.float32))
    running = jnp.zeros((TOKENS, D), jnp.float32)
    differences = []
    for layer in range(L):
        running = running + writes[layer]
        differences.append(running - mlp_outputs[layer].astype(jnp.float32))
    later = jnp.zeros((TOKENS, D), jnp.float32)
    grads = [None] * L
    for layer in range(L - 1, -1, -1):
        later = later + differences[layer]
        signal = later.astype(jnp.bfloat16)
        total = jnp.dot(latents[layer].T, signal, preferred_element_type=jnp.float32)
        grads[layer] = (total / TOKENS).astype(jnp.bfloat16)
    return jnp.stack(differences).astype(jnp.bfloat16), jnp.stack(grads)
```

```python
import jax
import jax.numpy as jnp
from jax import lax
from jax.sharding import Mesh
from jax.sharding import PartitionSpec as P


CHUNKS = 2
STEPS = (0, -1, 1, 2)


def unpack_words(words):
    shifts = jnp.arange(16, dtype=jnp.int32)
    bits = jnp.right_shift(words[..., None], shifts) & 1
    return bits.reshape(words.shape[:-1] + (words.shape[-1] * 16,))


def ring_pairs(size, way):
    pairs = []
    for p in range(size):
        for c in range(2):
            step = way if c == 0 else -way
            pairs.append((p * 2 + c, ((p + step) % size) * 2 + c))
    return pairs


def ahead(v, axis):
    return lax.ppermute(v, (axis, "c"), ring_pairs(4, 1))


def back(v, axis):
    return lax.ppermute(v, (axis, "c"), ring_pairs(4, -1))


def partner(v):
    return lax.ppermute(v, "c", [(0, 1), (1, 0)])


def sibling(v):
    return lax.ppermute(v, "zl", [(0, 1), (1, 0)])


def shift_y(v, k):
    return lax.ppermute(v, "y", [(i, (i + k) % 4) for i in range(4)])


def ring_gather(v, axis):
    behind = ahead(v, axis)
    front = back(v, axis)
    far = ahead(behind, axis)
    return [v, behind, front, far]


def plane_gather(v):
    z = ring_gather(v, "zh")
    g0 = ring_gather(z[0], "x")
    near = jnp.concatenate([z[1], z[2]], axis=0)
    g1 = ring_gather(near, "x")
    g2 = ring_gather(z[3], "x")
    return [jnp.concatenate([g0[i], g1[i], g2[i]], axis=0) for i in range(4)]


def ring_reduce(own, behind, front, far, axis, kind):
    up = ahead(far.astype(kind), axis)
    down = back(behind.astype(kind), axis)
    mid = ahead((front + up.astype(jnp.float32)).astype(kind), axis)
    return own + down.astype(jnp.float32) + mid.astype(jnp.float32)


def local(mlp_inputs, mlp_outputs, encoder, encoder_bias, active_words, decoder):
    f32 = jnp.float32
    bf16 = jnp.bfloat16
    x_in = mlp_inputs[0]
    target = mlp_outputs[0]
    rows, width = x_in.shape
    xi = lax.axis_index("x")
    zi = lax.axis_index("zh")
    ci = lax.axis_index("c")
    yi = lax.axis_index("y")
    li = lax.axis_index("zl")
    layer = yi * 2 + li

    enc_a = encoder[0]
    dec_a = decoder[0]
    enc_b = partner(enc_a)
    dec_b = partner(dec_a)
    bias_a = encoder_bias
    bias_b = partner(bias_a)
    target_b = sibling(target)

    xs = plane_gather(x_in)

    half = rows * 16
    tokens = 2 * half
    steps = jnp.array(STEPS, jnp.int32)

    def picker(core):
        sign = 1 - 2 * core
        xo = (xi + sign * steps) % 4
        zo = (zi + sign * steps) % 4
        base = (xo[:, None] * 8 + zo[None, :] * 2).reshape(16)
        ids = ((base + core) * rows)[:, None] + jnp.arange(rows, dtype=jnp.int32)[None, :]
        return (ids.reshape(half)[:, None] == jnp.arange(tokens, dtype=jnp.int32)[None, :]).astype(bf16)

    bits = unpack_words(active_words[0]).astype(bf16)
    gate_a = jnp.dot(picker(ci), bits, preferred_element_type=f32).astype(bf16)
    gate_b = partner(jnp.dot(picker(1 - ci), bits, preferred_element_type=f32).astype(bf16))

    def latents(i):
        part = slice(i * rows * 4, (i + 1) * rows * 4)

        def one(enc, bias, gate):
            pre = jnp.dot(xs[i], enc, preferred_element_type=f32) + bias
            return (gate[part].astype(f32) * pre).astype(bf16)

        return one(enc_a, bias_a, gate_a), one(enc_b, bias_b, gate_b)

    lat = [latents(i) for i in range(4)]
    lat_a = jnp.concatenate([a for a, _ in lat], axis=0)
    lat_far = partner(jnp.concatenate([b for _, b in lat], axis=0))
    lat_full = [jnp.concatenate([a, b], axis=1) for a, b in lat]
    dec = jnp.concatenate([dec_a, dec_b], axis=0)

    step = width // CHUNKS
    errors = []
    grads = []
    m_me_all = target.astype(f32)
    m_pt_all = target_b.astype(f32)
    weight = (8 - layer).astype(f32)
    low = li.astype(f32)

    for j in range(CHUNKS):
        cols = slice(j * step, (j + 1) * step)
        dec_j = dec[:, cols]
        part = [jnp.dot(lat_full[i], dec_j, preferred_element_type=f32) for i in range(4)]
        acc = ring_reduce(part[0], part[1], part[2], part[3], "x", bf16)
        zs = [acc[i * rows : (i + 1) * rows] for i in range(4)]
        mine = ring_reduce(zs[0], zs[1], zs[2], zs[3], "zh", f32)
        other = sibling(mine)
        m_me = m_me_all[:, cols]
        m_pt = m_pt_all[:, cols]
        w_pair = mine + other
        pt_weight = jnp.where(li == 0, weight - 1.0, weight + 1.0)
        v_pair = weight * mine + pt_weight * other - m_me - m_pt
        got1 = shift_y(jnp.where(yi == 3, v_pair, w_pair), 1)
        got3 = shift_y(jnp.where(yi == 0, w_pair, v_pair), -1)
        got2 = shift_y(jnp.where(yi >= 2, v_pair, w_pair), 2)
        zero = jnp.zeros_like(mine)
        lower = (
            jnp.where(yi >= 1, got1, zero) + jnp.where(yi == 3, got3, zero) + jnp.where(yi >= 2, got2, zero)
        )
        upper = (
            jnp.where(yi >= 1, zero, got1) + jnp.where(yi == 3, zero, got3) + jnp.where(yi >= 2, zero, got2)
        )
        recon = lower + mine + low * other
        difference = recon - m_me
        later = weight * recon - m_me + upper + (1.0 - low) * (pt_weight * other - m_pt)
        errors.append(difference.astype(bf16))
        signal = later.astype(bf16)
        sig_a = jnp.concatenate(plane_gather(signal), axis=0)
        sig_b = partner(sig_a)
        dims = (((0,), (0,)), ((), ()))
        total = lax.dot_general(lat_a, sig_a, dims, preferred_element_type=f32) + lax.dot_general(
            lat_far, sig_b, dims, preferred_element_type=f32
        )
        grads.append((total / tokens).astype(bf16))
    return (
        jnp.concatenate(errors, axis=1)[None],
        jnp.concatenate(grads, axis=1)[None],
    )


def solution(mesh):
    names = ("y", "zl", "x", "zh", "c")
    split = Mesh(mesh.devices.reshape(4, 2, 4, 4, 2), names)
    layer = ("y", "zl")
    place = ("x", "zh", "c")
    placed = (
        P(layer, place, None),
        P(layer, place, None),
        P(layer, None, place),
        P(layer, place),
        P(layer, None, place),
        P(layer, place, None),
    )
    return jax.shard_map(
        local,
        mesh=split,
        in_specs=placed,
        out_specs=(P(layer, place, None), P(layer, place, None)),
        check_vma=False,
    )
```

```python
import jax
import jax.numpy as jnp
from jax import lax
from jax.sharding import Mesh
from jax.sharding import PartitionSpec as P


WIDTHS = (1920, 2176)
STEPS = (0, -1, 1, 2)


def unpack_words(words):
    shifts = jnp.arange(16, dtype=jnp.int32)
    bits = jnp.right_shift(words[..., None], shifts) & 1
    return bits.reshape(words.shape[:-1] + (words.shape[-1] * 16,))


def ring_pairs(size, way):
    pairs = []
    for p in range(size):
        for c in range(2):
            step = way if c == 0 else -way
            pairs.append((p * 2 + c, ((p + step) % size) * 2 + c))
    return pairs


def ahead(v, axis):
    return lax.ppermute(v, (axis, "c"), ring_pairs(4, 1))


def back(v, axis):
    return lax.ppermute(v, (axis, "c"), ring_pairs(4, -1))


def partner(v):
    return lax.ppermute(v, "c", [(0, 1), (1, 0)])


def sibling(v):
    return lax.ppermute(v, "zl", [(0, 1), (1, 0)])


def shift_y(v, k):
    return lax.ppermute(v, "y", [(i, (i + k) % 4) for i in range(4)])


def ring_gather(v, axis):
    behind = ahead(v, axis)
    front = back(v, axis)
    far = ahead(behind, axis)
    return [v, behind, front, far]


def plane_gather_fine(v):
    z = ring_gather(v, "zh")
    g0 = ring_gather(z[0], "x")
    near = jnp.concatenate([z[1], z[2]], axis=0)
    g1 = ring_gather(near, "x")
    g2 = ring_gather(z[3], "x")
    return [jnp.concatenate([g0[i], g1[i], g2[i]], axis=0) for i in range(4)]


def plane_gather(v):
    row = jnp.concatenate(ring_gather(v, "zh"), axis=0)
    return ring_gather(row, "x")


def ring_reduce(own, behind, front, far, axis, kind):
    up = ahead(far.astype(kind), axis)
    down = back(behind.astype(kind), axis)
    mid = ahead((front + up.astype(jnp.float32)).astype(kind), axis)
    return own + down.astype(jnp.float32) + mid.astype(jnp.float32)


def body(mlp_inputs, mlp_outputs, encoder, encoder_bias, active_words, decoder):
    f32 = jnp.float32
    bf16 = jnp.bfloat16
    x_in = mlp_inputs[0]
    target = mlp_outputs[0]
    rows, _ = x_in.shape
    xi = lax.axis_index("x")
    zi = lax.axis_index("zh")
    ci = lax.axis_index("c")
    yi = lax.axis_index("y")
    li = lax.axis_index("zl")
    layer = yi * 2 + li

    enc_a = encoder[0]
    dec_a = decoder[0]
    enc_b = partner(enc_a)
    dec_b = partner(dec_a)
    bias_a = encoder_bias
    bias_b = partner(bias_a)
    target_b = sibling(target)

    xs = plane_gather_fine(x_in)

    half = rows * 16
    tokens = 2 * half
    steps = jnp.array(STEPS, jnp.int32)

    def picker(core):
        sign = 1 - 2 * core
        xo = (xi + sign * steps) % 4
        zo = (zi + sign * steps) % 4
        base = (xo[:, None] * 8 + zo[None, :] * 2).reshape(16)
        ids = ((base + core) * rows)[:, None] + jnp.arange(rows, dtype=jnp.int32)[None, :]
        return (ids.reshape(half)[:, None] == jnp.arange(tokens, dtype=jnp.int32)[None, :]).astype(bf16)

    bits = unpack_words(active_words[0]).astype(bf16)
    gate_a = jnp.dot(picker(ci), bits, preferred_element_type=f32).astype(bf16)
    gate_b = partner(jnp.dot(picker(1 - ci), bits, preferred_element_type=f32).astype(bf16))

    enc = jnp.concatenate([enc_a, enc_b], axis=1)
    dec = jnp.concatenate([dec_a, dec_b], axis=0)
    bias = jnp.concatenate([bias_a, bias_b], axis=1)
    gate = jnp.concatenate([gate_a, gate_b], axis=1)

    def latents(i):
        pre = jnp.dot(xs[i], enc, preferred_element_type=f32) + bias
        return (gate[i * rows * 4 : (i + 1) * rows * 4].astype(f32) * pre).astype(bf16)

    lat_full = [latents(i) for i in range(4)]
    cut = encoder.shape[2]
    lat_a = jnp.concatenate([v[:, :cut] for v in lat_full], axis=0)
    lat_far = partner(jnp.concatenate([v[:, cut:] for v in lat_full], axis=0))

    starts = (0, WIDTHS[0])
    errors = []
    grads = []
    weight = (8 - layer).astype(f32)
    low = li.astype(f32)

    for j, step in enumerate(WIDTHS):
        cols = slice(starts[j], starts[j] + step)
        dec_j = dec[:, cols]
        part = []
        for i in range(4):
            part.append(jnp.dot(lat_full[i], dec_j, preferred_element_type=f32))
        acc = ring_reduce(part[0], part[1], part[2], part[3], "x", bf16)
        zs = [acc[i * rows : (i + 1) * rows] for i in range(4)]
        mine = ring_reduce(zs[0], zs[1], zs[2], zs[3], "zh", bf16)
        other = sibling(mine.astype(bf16)).astype(f32)
        m_me = target[:, cols].astype(f32)
        m_pt = target_b[:, cols].astype(f32)
        w_pair = mine + other
        pt_weight = jnp.where(li == 0, weight - 1.0, weight + 1.0)
        v_pair = weight * mine + pt_weight * other - m_me - m_pt
        w_pair = w_pair.astype(bf16)
        v_pair = v_pair.astype(bf16)
        got1 = shift_y(jnp.where(yi == 3, v_pair, w_pair), 1).astype(f32)
        got3 = shift_y(jnp.where(yi == 0, w_pair, v_pair), -1).astype(f32)
        got2 = shift_y(jnp.where(yi >= 2, v_pair, w_pair), 2).astype(f32)
        zero = jnp.zeros_like(mine)
        lower = (
            jnp.where(yi >= 1, got1, zero) + jnp.where(yi == 3, got3, zero) + jnp.where(yi >= 2, got2, zero)
        )
        upper = (
            jnp.where(yi >= 1, zero, got1) + jnp.where(yi == 3, zero, got3) + jnp.where(yi >= 2, zero, got2)
        )
        recon = lower + mine + low * other
        difference = recon - m_me
        later = weight * recon - m_me + upper + (1.0 - low) * (pt_weight * other - m_pt)
        errors.append(difference.astype(bf16))
        signal = later.astype(bf16)
        sig_a = jnp.concatenate(plane_gather(signal), axis=0)
        sig_b = partner(sig_a)
        dims = (((0,), (0,)), ((), ()))
        total = lax.dot_general(lat_far, sig_b, dims, preferred_element_type=f32)
        total = total + lax.dot_general(lat_a, sig_a, dims, preferred_element_type=f32)
        grads.append((total / tokens).astype(bf16))
    error = jnp.concatenate(errors, axis=1)
    return (
        error[None],
        jnp.concatenate(grads, axis=1)[None],
    )


def solution(mesh):
    names = ("y", "zl", "x", "zh", "c")
    split = Mesh(mesh.devices.reshape(4, 2, 4, 4, 2), names)
    layer = ("y", "zl")
    place = ("x", "zh", "c")
    placed = (
        P(layer, place, None),
        P(layer, place, None),
        P(layer, None, place),
        P(layer, place),
        P(layer, None, place),
        P(layer, place, None),
    )
    return jax.shard_map(
        body,
        mesh=split,
        in_specs=placed,
        out_specs=(P(layer, place, None), P(layer, place, None)),
        check_vma=False,
    )
```
